16 devices in a mesh: dp: 1, tp: 16 (over x, y, z, core).
Axes of the slice: x: 2, y: 2, z: 2, core: 2. Of those that a mesh axis runs over, the one named last changes fastest.
Arguments:
- x: bfloat16 [2048, 4096], P('dp')
- dy: bfloat16 [2048, 4096], P('dp')
- gate: bfloat16 [2048, 12288], P('dp', 'tp')
- up: bfloat16 [2048, 12288], P('dp', 'tp')
- w_gate: bfloat16 [4096, 12288], P(None, 'tp')
- w_up: bfloat16 [4096, 12288], P(None, 'tp')
- w_down: bfloat16 [12288, 4096], P('tp')
Outputs:
- output 1: bfloat16 [2048, 4096], P('dp')
- output 2: bfloat16 [4096, 12288], P('dp', 'tp')
- output 3: bfloat16 [4096, 12288], P('dp', 'tp')
- output 4: bfloat16 [12288, 4096], P(('dp', 'tp'))
All inputs are finite; a program needn't handle non-finite values.
Results may differ from the reference program's by a relative error of at most 0.012.
Values are sent between devices in bfloat16 or wider.
A program may use at most 2 GiB of HBM per device.

```python
import jax
import jax.numpy as jnp

ROWS = 2048
D = 4096
FF = 12288


def act(gate, up):
    return jax.nn.silu(gate) * up


def setup_inputs(seed: int = 0, part: int = 0) -> dict:
    kx, ky, ka, kb, kg, ku, kd = jax.random.split(jax.random.key(seed), 7)
    kx, ky, ka, kb = (jax.random.fold_in(k, part) for k in (kx, ky, ka, kb))
    drawn = {
        "x": jax.random.normal(kx, (ROWS, D), jnp.float32),
        "dy": jax.random.normal(ky, (ROWS, D), jnp.float32),
        "gate": jax.random.normal(ka, (ROWS, FF), jnp.float32),
        "up": jax.random.normal(kb, (ROWS, FF), jnp.float32),
        "w_gate": jax.random.normal(kg, (D, FF), jnp.float32) * D**-0.5,
        "w_up": jax.random.normal(ku, (D, FF), jnp.float32) * D**-0.5,
        "w_down": jax.random.normal(kd, (FF, D), jnp.float32) * FF**-0.5,
    }
    return {k: v.astype(jnp.bfloat16) for k, v in drawn.items()}


def reference(x, dy, gate, up, w_gate, w_up, w_down):
    hidden, back = jax.vjp(act, gate.astype(jnp.float32), up.astype(jnp.float32))
    d_hidden = jnp.dot(dy, w_down.T, preferred_element_type=jnp.float32)
    d_gate, d_up = (g.astype(jnp.bfloat16) for g in back(d_hidden))
    dx = jnp.dot(d_gate, w_gate.T, preferred_element_type=jnp.float32) + jnp.dot(d_up, w_up.T, preferred_element_type=jnp.float32)
    dw_gate = jnp.dot(x.T, d_gate, preferred_element_type=jnp.float32)
    dw_up = jnp.dot(x.T, d_up, preferred_element_type=jnp.float32)
    dw_down = jnp.dot(hidden.astype(jnp.bfloat16).T, dy, preferred_element_type=jnp.float32)
    return tuple(g.astype(jnp.bfloat16) for g in (dx, dw_gate, dw_up, dw_down))
```

```python
import jax
import jax.numpy as jnp
from jax import lax
from jax.experimental import pallas as pl
from jax.experimental.pallas import tpu as pltpu
from jax.sharding import PartitionSpec as P

bf16, f32 = jnp.bfloat16, jnp.float32
MESH = pl.DeviceIdType.MESH
ROWS, D, FF = 2048, 4096, 768
CHUNKS, R = 8, 256
HALF = D // 2
OFF, WIDTH = (0, 768, 1536), (768, 768, 512)
GROUPS = range(3)
TILE = 256
NB = 1024
AG3 = ((0, 1, 2), (3, 4), (5,), (6,), (7,), (), (), ())
AG2 = ((), (0, 1), (2,), (3,), (4,), (5, 6), (7,), ())
AG1 = ((), (), (), (0,), (1,), (2,), (3,), (4,))


def dot(a, b, ca, cb):
    return lax.dot_general(a, b, (((ca,), (cb,)), ((), ())), preferred_element_type=f32)


def kernel(
    x, dy, gate, up, wg, wu, wd,
    dx, dwg, dwu, dwd,
    dg, du, hid, dyb, ring, acc, kp1, kp2, s1, s2, s3, r1, r2, r3,
    dy_sem, w_sem, xd_sem, ss, rs, free,
):
    me = lax.axis_index("tp")
    core = lax.rem(me, 2)
    bits = tuple(lax.rem(me // s, 2) for s in (8, 4, 2))
    other = me + 1 - 2 * core

    def pick(r, values):
        return jnp.where(r == 0, values[0], jnp.where(r == 1, values[1], values[2]))

    peers = tuple(me + s * (1 - 2 * b) for s, b in zip((8, 4, 2), bits))

    def chunk_copies(k):
        rows = pl.ds(pl.multiple_of(k * R, R), R)
        return [
            pltpu.make_async_copy(dy.at[rows, :], dyb, dy_sem.at[0]),
            pltpu.make_async_copy(gate.at[rows, :], hid.at[rows, :], dy_sem.at[1]),
            pltpu.make_async_copy(up.at[rows, :], du.at[rows, :], dy_sem.at[2]),
        ]

    def w_copies(half, i):
        rows = pl.ds(pl.multiple_of(half * HALF, HALF), HALF)
        return [pltpu.make_async_copy(a.at[rows, :], b.at[rows, :], w_sem.at[i, n]) for n, (a, b) in enumerate(((wg, dwg), (wu, dwu)))]

    def xd_copy(t, which):
        i = 2 * t + which
        cols = pl.ds(pl.multiple_of(t * TILE, TILE), TILE)
        return pltpu.make_async_copy((x, dy)[which].at[:, cols], ring.at[lax.rem(i, 3)], xd_sem.at[lax.rem(i, 3)])

    wd_copy = pltpu.make_async_copy(wd, dwd, w_sem.at[2, 0])
    first = chunk_copies(0)
    first[0].start()
    wd_copy.start()
    first[1].start()
    first[2].start()
    for c in w_copies(1 - core, 0) + w_copies(core, 1):
        c.start()

    barrier = pltpu.get_barrier_semaphore()
    for p in peers + (other,):
        pl.semaphore_signal(barrier, inc=1, device_id={"tp": p}, device_id_type=MESH)
    pl.semaphore_wait(barrier, 4)

    def remote(kind, k, g, src, dst, to):
        return pltpu.make_async_remote_copy(
            src_ref=src, dst_ref=dst, send_sem=ss.at[kind, k, g], recv_sem=rs.at[kind, k, g],
            device_id={"tp": to}, device_id_type=MESH,
        )

    def place(k, g):
        o = [lax.rem(g + k + i, 3) for i in range(3)]
        b = [pick(r, bits) for r in o]
        p = [pick(r, peers) for r in o]
        keep1 = k * R + b[0] * 128
        send1 = k * R + (1 - b[0]) * 128
        keep2, send2 = keep1 + b[1] * 64, keep1 + (1 - b[1]) * 64
        keep3, send3 = keep2 + b[2] * 32, keep2 + (1 - b[2]) * 32
        return b, p, (keep1, keep2, keep3), (send1, send2, send3)

    def mine(start, n, g):
        return dx.at[pl.ds(pl.multiple_of(start, 32), n), pl.ds(pl.multiple_of(core * HALF + OFF[g], 256), WIDTH[g])]

    def theirs(k, g):
        return dx.at[pl.ds(pl.multiple_of(k * R, R), R), pl.ds(pl.multiple_of((1 - core) * HALF + OFF[g], 256), WIDTH[g])]

    def copy_of(kind, k, g):
        b, p, keep, send = place(k, g)
        cols = pl.ds(OFF[g], WIDTH[g])
        if kind == 0:
            return remote(0, k, g, theirs(k, g), theirs(k, g), other)
        if kind == 1:
            return remote(1, k, g, s1.at[:, cols], r1.at[k, :, cols], p[0])
        if kind == 2:
            return remote(2, k, g, s2.at[:, cols], r2.at[k, :, cols], p[1])
        if kind == 3:
            return remote(3, k, g, s3.at[:, cols], r3.at[k, :, cols], p[2])
        if kind == 4:
            return remote(4, k, g, mine(keep[2], 32, g), mine(keep[2], 32, g), p[2])
        if kind == 5:
            return remote(5, k, g, mine(keep[1], 64, g), mine(keep[1], 64, g), p[1])
        if kind == 6:
            return remote(6, k, g, mine(keep[0], 128, g), mine(keep[0], 128, g), p[0])
        if kind == 7:
            return remote(7, k, g, mine(keep[1], 64, g), mine(keep[1], 64, g), other)
        if kind == 8:
            return remote(8, k, g, mine(send[1], 64, g), mine(send[1], 64, g), other)
        return remote(9, k, g, mine(send[0], 128, g), mine(send[0], 128, g), other)

    def slot_of(k):
        return lax.rem(k, 2)

    def sent(kind, k, g):
        @pl.when(k >= 1)
        def _():
            copy_of(kind, k - 1, g).wait_send()

    def after_own(k, g):
        b, p, keep, send = place(k, g)
        s, cols, w = slot_of(k), pl.ds(OFF[g], WIDTH[g]), WIDTH[g]
        copy_of(0, k, g).wait_recv()
        sent(1, k, g)
        for i in range(0, 128, 32):
            v = acc[pl.ds(pl.multiple_of((1 - b[0]) * 128 + i, 32), 32), cols]
            s1[pl.ds(i, 32), cols] = (v + mine(send[0] + i, 32, g)[...].astype(f32)).astype(bf16)
        copy_of(1, k, g).start()
        for i in range(0, 128, 32):
            v = acc[pl.ds(pl.multiple_of(b[0] * 128 + i, 32), 32), cols]
            kp1[s, pl.ds(i, 32), cols] = v + mine(keep[0] + i, 32, g)[...].astype(f32)

    def rs1(k, g):
        b, p, keep, send = place(k, g)
        s, cols = slot_of(k), pl.ds(OFF[g], WIDTH[g])
        copy_of(1, k, g).wait_recv()
        sent(2, k, g)
        for i in range(0, 64, 32):
            rows = pl.ds(pl.multiple_of((1 - b[1]) * 64 + i, 32), 32)
            s2[pl.ds(i, 32), cols] = (kp1[s, rows, cols] + r1[k, rows, cols].astype(f32)).astype(bf16)
        copy_of(2, k, g).start()
        for i in range(0, 64, 32):
            rows = pl.ds(pl.multiple_of(b[1] * 64 + i, 32), 32)
            kp2[s, pl.ds(i, 32), cols] = kp1[s, rows, cols] + r1[k, rows, cols].astype(f32)

    def rs2(k, g):
        b, p, keep, send = place(k, g)
        s, cols = slot_of(k), pl.ds(OFF[g], WIDTH[g])
        copy_of(2, k, g).wait_recv()
        sent(3, k, g)
        there = pl.ds(pl.multiple_of((1 - b[2]) * 32, 32), 32)
        here = pl.ds(pl.multiple_of(b[2] * 32, 32), 32)
        s3[:, cols] = (kp2[s, there, cols] + r2[k, there, cols].astype(f32)).astype(bf16)
        copy_of(3, k, g).start()
        kp2[s, here, cols] = kp2[s, here, cols] + r2[k, here, cols].astype(f32)

    def rs3(k, g):
        b, p, keep, send = place(k, g)
        s, cols = slot_of(k), pl.ds(OFF[g], WIDTH[g])
        copy_of(3, k, g).wait_recv()
        here = pl.ds(pl.multiple_of(b[2] * 32, 32), 32)
        mine(keep[2], 32, g)[...] = (kp2[s, here, cols] + r3[k, :, cols].astype(f32)).astype(bf16)
        copy_of(4, k, g).start()

    def ag3(k, g):
        copy_of(4, k, g).wait_recv()
        copy_of(5, k, g).start()
        copy_of(7, k, g).start()

    def ag2(k, g):
        copy_of(5, k, g).wait_recv()
        copy_of(6, k, g).start()
        copy_of(8, k, g).start()

    def ag1(k, g):
        copy_of(6, k, g).wait_recv()
        copy_of(9, k, g).start()

    def all_groups(event, k):
        if event is ag3:
            pl.semaphore_wait(free.at[k], 1)
        for g in GROUPS:
            event(k, g)

    def halving(k):
        @pl.when(jnp.logical_and(k >= 3, k < 11))
        def _():
            all_groups(rs3, k - 3)

        @pl.when(jnp.logical_and(k >= 2, k < 10))
        def _():
            all_groups(rs2, k - 2)

        @pl.when(jnp.logical_and(k >= 1, k < 9))
        def _():
            all_groups(rs1, k - 1)

    wd_copy.wait()

    @pl.loop(0, CHUNKS)
    def _(k):
        rows = pl.ds(pl.multiple_of(k * R, R), R)
        for c in chunk_copies(k):
            c.wait()
        acc[:, pl.ds(0, FF)] = dot(dyb[...], dwd[...], 1, 1)

        @pl.loop(0, R // 16)
        def _(i):
            block = pl.ds(pl.multiple_of(i * 16, 16), 16)
            here = pl.ds(pl.multiple_of(k * R + i * 16, 16), 16)
            a, b, d = hid[here, :].astype(f32), du[here, :].astype(f32), acc[block, pl.ds(0, FF)]
            sig = jax.nn.sigmoid(a)
            silu = a * sig
            hid[here, :] = (silu * b).astype(bf16)
            du[here, :] = (d * silu).astype(bf16)
            dg[here, :] = (d * b * (sig + silu * (1.0 - sig))).astype(bf16)

        @pl.when(k < CHUNKS - 1)
        def _():
            for c in chunk_copies(k + 1):
                c.start()

        @pl.when(k == CHUNKS - 1)
        def _():
            for i in range(3):
                xd_copy(i // 2, i % 2).start()

        @pl.when(k == 0)
        def _():
            for c in w_copies(1 - core, 0):
                c.wait()

        for n in range(0, HALF, NB):
            w = pl.ds(pl.multiple_of((1 - core) * HALF + n, 256), NB)
            acc[:, pl.ds(n, NB)] = dot(dg[rows, :], dwg[w, :], 1, 1) + dot(du[rows, :], dwu[w, :], 1, 1)
        for g in GROUPS:
            ref = theirs(k, g)
            for i in range(0, R, 32):
                ref[pl.ds(i, 32), :] = acc[pl.ds(i, 32), pl.ds(OFF[g], WIDTH[g])].astype(bf16)
            copy_of(0, k, g).start()

        @pl.when(k == 0)
        def _():
            for c in w_copies(core, 1):
                c.wait()

        for n in range(0, HALF, NB):
            w = pl.ds(pl.multiple_of(core * HALF + n, 256), NB)
            acc[:, pl.ds(n, NB)] = dot(dg[rows, :], dwg[w, :], 1, 1) + dot(du[rows, :], dwu[w, :], 1, 1)
        for g in GROUPS:
            after_own(k, g)

        for g in GROUPS:
            copy_of(0, k, g).wait_send()
        pl.semaphore_signal(free.at[k], inc=1, device_id={"tp": other}, device_id_type=MESH)
        halving(k)

    @pl.loop(0, 8)
    def _(u):
        for s in range(2):
            t = 2 * u + s
            tile = pl.ds(pl.multiple_of(t * TILE, TILE), TILE)
            xd_copy(t, 0).wait()
            xt, yt = ring.at[lax.rem(2 * t, 3)], ring.at[lax.rem(2 * t + 1, 3)]
            dwg[tile, :] = dot(xt[...], dg[...], 0, 0).astype(bf16)
            if s == 0:
                halving(8 + u)
            dwu[tile, :] = dot(xt[...], du[...], 0, 0).astype(bf16)

            @pl.when(t < 15)
            def _():
                xd_copy(t + 1, 1).start()

            xd_copy(t, 1).wait()
            if s == 1:
                for i in range(8):
                    if AG3[i] + AG2[i] + AG1[i]:
                        @pl.when(u == i)
                        def _():
                            for k in AG3[i]:
                                all_groups(ag3, k)
                            for k in AG2[i]:
                                all_groups(ag2, k)
                            for k in AG1[i]:
                                all_groups(ag1, k)
            dwd[:, tile] = dot(hid[...], yt[...], 0, 0).astype(bf16)

            @pl.when(t < 14)
            def _():
                xd_copy(t + 2, 0).start()

    for k in range(5, 8):
        all_groups(ag1, k)

    @pl.loop(0, CHUNKS)
    def _(k):
        for g in GROUPS:
            for kind in range(4, 10):
                if kind >= 7:
                    copy_of(kind, k, g).wait_recv()
                copy_of(kind, k, g).wait_send()

    for g in GROUPS:
        for kind in range(1, 4):
            copy_of(kind, CHUNKS - 1, g).wait_send()


def solution(mesh):
    hbm = pl.BlockSpec(memory_space=pltpu.HBM)
    vmem = pl.BlockSpec(memory_space=pltpu.VMEM)
    sem = pltpu.SemaphoreType.DMA

    def step(*args):
        return tuple(pl.pallas_call(
            kernel,
            out_shape=[pltpu.VMEM(s, bf16) for s in ((ROWS, D), (D, FF), (D, FF), (FF, D))],
            in_specs=[hbm] * 7,
            out_specs=[vmem] * 4,
            scratch_shapes=[
                pltpu.VMEM((ROWS, FF), bf16),
                pltpu.VMEM((ROWS, FF), bf16),
                pltpu.VMEM((ROWS, FF), bf16),
                pltpu.VMEM((R, D), bf16),
                pltpu.VMEM((3, ROWS, TILE), bf16),
                pltpu.VMEM((R, HALF), f32),
                pltpu.VMEM((2, 128, HALF), f32),
                pltpu.VMEM((2, 64, HALF), f32),
                pltpu.VMEM((128, HALF), bf16),
                pltpu.VMEM((64, HALF), bf16),
                pltpu.VMEM((32, HALF), bf16),
                pltpu.VMEM((CHUNKS, 128, HALF), bf16),
                pltpu.VMEM((CHUNKS, 64, HALF), bf16),
                pltpu.VMEM((CHUNKS, 32, HALF), bf16),
                sem((3,)), sem((3, 2)), sem((3,)),
                sem((10, CHUNKS, 3)), sem((10, CHUNKS, 3)), pltpu.SemaphoreType.REGULAR((CHUNKS,)),
            ],
            compiler_params=pltpu.CompilerParams(collective_id=0, has_side_effects=True, vmem_limit_bytes=VMEM_LIMIT),
        )(*args))

    tokens, columns, rows = P("dp", None), P(None, "tp"), P("tp", None)
    return jax.shard_map(
        step,
        mesh=mesh,
        in_specs=(tokens, tokens, P("dp", "tp"), P("dp", "tp"), columns, columns, rows),
        out_specs=(tokens, P("dp", "tp"), P("dp", "tp"), P(("dp", "tp"), None)),
        check_vma=False,
    )


VMEM_LIMIT = 31_391_744
```

```python
import jax
import jax.numpy as jnp
from jax import lax
from jax.experimental import pallas as pl
from jax.experimental.pallas import tpu as pltpu
from jax.sharding import PartitionSpec as P

bf16, f32 = jnp.bfloat16, jnp.float32
MESH = pl.DeviceIdType.MESH
ROWS, D, FF = 2048, 4096, 768
CHUNKS, R = 8, 256
HALF = D // 2
OFF, WIDTH = (0, 768, 1536), (768, 768, 512)
GROUPS = range(3)
TILE = 256
STRIP = 16
NB = 1024
KEPT = 4
PHASE1 = {
    (2, "b"): [("rs1", 0)],
    (2, "o"): [("rs1", 1)],
    (3, "b"): [("rs2", 0)],
    (3, "o"): [("rs1", 2)],
    (4, "b"): [("rs2", 1), ("rs3", 0)],
    (4, "o"): [("rs1", 3)],
    (5, "b"): [("rs3", 1), ("rs2", 2)],
    (5, "g"): [("ag3", 0)],
    (5, "o"): [("rs1", 4)],
    (6, "b"): [("rs2", 3), ("ag3", 1)],
    (6, "g"): [("rs3", 2)],
    (6, "o"): [("ag2", 0)],
    (7, "b"): [("rs1", 5)],
    (7, "o"): [("rs3", 3), ("rs2", 4)],
}
PHASE2 = {
    (0, "a"): [("ag3", 2), ("ag2", 1)],
    (1, "a"): [("rs1", 6), ("ag1", 0)],
    (3, "a"): [("rs2", 5)],
    (3, "b"): [("ag3", 3)],
    (4, "a"): [("rs3", 4)],
    (4, "b"): [("ag2", 2)],
    (6, "a"): [("rs1", 7), ("ag1", 1)],
    (6, "b"): [("rs2", 6)],
    (7, "a"): [("rs3", 5)],
    (7, "b"): [("ag2", 3)],
    (8, "a"): [("ag3", 4)],
    (9, "a"): [("rs2", 7), ("ag1", 2)],
    (9, "b"): [("rs3", 6)],
    (10, "a"): [("ag3", 5)],
    (11, "a"): [("ag1", 3)],
    (11, "b"): [("ag2", 4)],
    (12, "a"): [("rs3", 7), ("ag3", 6)],
    (13, "a"): [("ag2", 5)],
    (14, "a"): [("ag1", 4)],
    (14, "b"): [("ag3", 7)],
    (15, "a"): [("ag2", 6)],
}
LAST = [("ag1", 5), ("ag2", 7), ("ag1", 6), ("ag1", 7)]


def dot(a, b, ca, cb):
    return lax.dot_general(a, b, (((ca,), (cb,)), ((), ())), preferred_element_type=f32)


def kernel(
    x, dy, gate, up, wg, wu, wd,
    dx, dwg, dwu, dwd,
    dg, du, hid, dyb, ring, acc, kp1, kp2, s1, s2, s3, r1,
    dy_sem, w_sem, xd_sem, ss, rs, free,
):
    me = lax.axis_index("tp")
    core = lax.rem(me, 2)
    bits = tuple(lax.rem(me // s, 2) for s in (8, 4, 2))
    other = me + 1 - 2 * core

    def pick(r, values):
        return jnp.where(r == 0, values[0], jnp.where(r == 1, values[1], values[2]))

    peers = tuple(me + s * (1 - 2 * b) for s, b in zip((8, 4, 2), bits))

    def chunk_copies(k):
        rows = pl.ds(pl.multiple_of(k * R, R), R)
        return [
            pltpu.make_async_copy(dy.at[rows, :], dyb, dy_sem.at[0]),
            pltpu.make_async_copy(gate.at[rows, :], hid.at[rows, :], dy_sem.at[1]),
            pltpu.make_async_copy(up.at[rows, :], du.at[rows, :], dy_sem.at[2]),
        ]

    def w_copies(half, i):
        rows = pl.ds(pl.multiple_of(half * HALF, HALF), HALF)
        return [pltpu.make_async_copy(a.at[rows, :], b.at[rows, :], w_sem.at[i, n]) for n, (a, b) in enumerate(((wg, dwg), (wu, dwu)))]

    def xd_copy(t, which):
        i = 2 * t + which
        cols = pl.ds(pl.multiple_of(t * TILE, TILE), TILE)
        return pltpu.make_async_copy((x, dy)[which].at[:, cols], ring.at[lax.rem(i, 3)], xd_sem.at[lax.rem(i, 3)])

    wd_copy = pltpu.make_async_copy(wd, dwd, w_sem.at[2, 0])
    first = chunk_copies(0)
    first[0].start()
    wd_copy.start()
    first[1].start()
    first[2].start()
    for c in w_copies(1 - core, 0) + w_copies(core, 1):
        c.start()

    barrier = pltpu.get_barrier_semaphore()
    for p in peers + (other,):
        pl.semaphore_signal(barrier, inc=1, device_id={"tp": p}, device_id_type=MESH)
    pl.semaphore_wait(barrier, 4)

    def remote(kind, k, g, src, dst, to):
        return pltpu.make_async_remote_copy(
            src_ref=src, dst_ref=dst, send_sem=ss.at[kind, k, g], recv_sem=rs.at[kind, k, g],
            device_id={"tp": to}, device_id_type=MESH,
        )

    def place(k, g):
        o = [lax.rem(g + k + i, 3) for i in range(3)]
        b = [pick(r, bits) for r in o]
        p = [pick(r, peers) for r in o]
        keep1 = k * R + b[0] * 128
        send1 = k * R + (1 - b[0]) * 128
        keep2, send2 = keep1 + b[1] * 64, keep1 + (1 - b[1]) * 64
        keep3, send3 = keep2 + b[2] * 32, keep2 + (1 - b[2]) * 32
        return b, p, (keep1, keep2, keep3), (send1, send2, send3)

    def mine(start, n, g):
        return dx.at[pl.ds(pl.multiple_of(start, STRIP), n), pl.ds(pl.multiple_of(core * HALF + OFF[g], 256), WIDTH[g])]

    def theirs(k, g):
        return dx.at[pl.ds(pl.multiple_of(k * R, R), R), pl.ds(pl.multiple_of((1 - core) * HALF + OFF[g], 256), WIDTH[g])]

    def copy_of(kind, k, g):
        b, p, keep, send = place(k, g)
        cols = pl.ds(OFF[g], WIDTH[g])
        if kind == 0:
            return remote(0, k, g, theirs(k, g), theirs(k, g), other)
        if kind == 1:
            return remote(1, k, g, s1.at[:, cols], r1.at[k, :, cols], p[0])
        if kind == 2:
            there = keep[0] + (1 - b[1]) * 64
            return remote(2, k, g, s2.at[:, cols], mine(there, 64, g), p[1])
        if kind == 3:
            return remote(3, k, g, s3.at[:, cols], r1.at[k, pl.ds(0, 32), cols], p[2])
        if kind == 4:
            return remote(4, k, g, mine(keep[2], 32, g), mine(keep[2], 32, g), p[2])
        if kind == 5:
            return remote(5, k, g, mine(keep[1], 64, g), mine(keep[1], 64, g), p[1])
        if kind == 6:
            return remote(6, k, g, mine(keep[0], 128, g), mine(keep[0], 128, g), p[0])
        if kind == 7:
            return remote(7, k, g, mine(keep[1], 64, g), mine(keep[1], 64, g), other)
        if kind == 8:
            return remote(8, k, g, mine(send[1], 64, g), mine(send[1], 64, g), other)
        return remote(9, k, g, mine(send[0], 128, g), mine(send[0], 128, g), other)

    def part(start, i):
        return pl.ds(pl.multiple_of(start + i, STRIP), STRIP)

    def event(kind, k, work=None, after=()):
        for g in GROUPS:
            copy_of(kind, k, g).wait_recv()
        if kind < 3 and k > 0:
            for g in GROUPS:
                copy_of(kind + 1, k - 1, g).wait_send()
        if work is not None:
            for g in GROUPS:
                work(k, g, pl.ds(OFF[g], WIDTH[g]), *place(k, g))
        for g in GROUPS:
            for n in after:
                copy_of(n, k, g).start()

    def own(k):
        for g in GROUPS:
            copy_of(0, k, g).wait_recv()

        @pl.when(k >= 1)
        def _():
            for g in GROUPS:
                copy_of(1, k - 1, g).wait_send()

        for g in GROUPS:
            b, p, keep, send = place(k, g)
            cols = pl.ds(OFF[g], WIDTH[g])
            for i in range(0, 128, STRIP):
                v = acc[part((1 - b[0]) * 128, i), cols] + mine(send[0] + i, STRIP, g)[...].astype(f32)
                s1[pl.ds(i, STRIP), cols] = v.astype(bf16)
                v = acc[part(b[0] * 128, i), cols] + mine(keep[0] + i, STRIP, g)[...].astype(f32)
                kp1[lax.rem(k, 2), pl.ds(i, STRIP), cols] = v
        for g in GROUPS:
            copy_of(1, k, g).start()

    def halve1(k, g, cols, b, p, keep, send):
        for i in range(0, 64, STRIP):
            rows = part((1 - b[1]) * 64, i)
            s2[pl.ds(i, STRIP), cols] = (kp1[k % 2, rows, cols] + r1[k, rows, cols].astype(f32)).astype(bf16)
            rows = part(b[1] * 64, i)
            kp2[k % KEPT, pl.ds(i, STRIP), cols] = kp1[k % 2, rows, cols] + r1[k, rows, cols].astype(f32)

    def halve2(k, g, cols, b, p, keep, send):
        for i in range(0, 32, STRIP):
            v = kp2[k % KEPT, part((1 - b[2]) * 32, i), cols] + mine(send[2] + i, STRIP, g)[...].astype(f32)
            s3[pl.ds(i, STRIP), cols] = v.astype(bf16)
            rows = part(b[2] * 32, i)
            kp2[k % KEPT, rows, cols] = kp2[k % KEPT, rows, cols] + mine(keep[2] + i, STRIP, g)[...].astype(f32)

    def halve3(k, g, cols, b, p, keep, send):
        for i in range(0, 32, STRIP):
            v = kp2[k % KEPT, part(b[2] * 32, i), cols] + r1[k, pl.ds(i, STRIP), cols].astype(f32)
            mine(keep[2] + i, STRIP, g)[...] = v.astype(bf16)

    def gather3(k):
        pl.semaphore_wait(free.at[k], 1)
        event(4, k, after=(5, 7))

    EVENTS = {
        "rs1": lambda k: event(1, k, halve1, (2,)),
        "rs2": lambda k: event(2, k, halve2, (3,)),
        "rs3": lambda k: event(3, k, halve3, (4,)),
        "ag3": gather3,
        "ag2": lambda k: event(5, k, after=(6, 8)),
        "ag1": lambda k: event(6, k, after=(9,)),
    }

    def exchanges(step, table, point):
        for (n, at), events in table.items():
            if at == point:
                @pl.when(step == n)
                def _():
                    for name, k in events:
                        EVENTS[name](k)

    def gradients(k):
        for c in chunk_copies(k):
            c.wait()
        acc[:, pl.ds(0, FF)] = dot(dyb[...], dwd[...], 1, 1)
        @pl.loop(0, R // 32)
        def _(n):
            i = pl.multiple_of(n * 32, 32)
            here = pl.ds(pl.multiple_of(k * R + i, 32), 32)
            a, b, d = hid[here, :].astype(f32), du[here, :].astype(f32), acc[pl.ds(i, 32), pl.ds(0, FF)]
            sig = jax.nn.sigmoid(a)
            silu = a * sig
            hid[here, :] = (silu * b).astype(bf16)
            du[here, :] = (d * silu).astype(bf16)
            dg[here, :] = (d * b * (sig + silu * (1.0 - sig))).astype(bf16)

    def term(k, half):
        rows = pl.ds(pl.multiple_of(k * R, R), R)
        @pl.loop(0, HALF // NB)
        def _(j):
            n = pl.multiple_of(j * NB, NB)
            w = pl.ds(pl.multiple_of(half * HALF + n, 256), NB)
            acc[:, pl.ds(n, NB)] = dot(dg[rows, :], dwg[w, :], 1, 1) + dot(du[rows, :], dwu[w, :], 1, 1)

    wd_copy.wait()
    gradients(0)
    for c in chunk_copies(1):
        c.start()
    for c in w_copies(1 - core, 0):
        c.wait()

    @pl.loop(0, CHUNKS)
    def _(k):
        term(k, 1 - core)
        for g in GROUPS:
            ref = theirs(k, g)
            for i in range(0, R, 32):
                ref[pl.ds(i, 32), :] = acc[pl.ds(i, 32), pl.ds(OFF[g], WIDTH[g])].astype(bf16)
        for g in GROUPS:
            copy_of(0, k, g).start()
        exchanges(k, PHASE1, "b")

        @pl.when(k < CHUNKS - 1)
        def _():
            gradients(k + 1)

        @pl.when(k < CHUNKS - 2)
        def _():
            for c in chunk_copies(k + 2):
                c.start()

        @pl.when(k == CHUNKS - 2)
        def _():
            for i in range(3):
                xd_copy(i // 2, i % 2).start()

        exchanges(k, PHASE1, "g")

        @pl.when(k == 0)
        def _():
            for c in w_copies(core, 1):
                c.wait()

        term(k, core)
        own(k)
        for g in GROUPS:
            copy_of(0, k, g).wait_send()
        pl.semaphore_signal(free.at[k], inc=1, device_id={"tp": other}, device_id_type=MESH)
        exchanges(k, PHASE1, "o")

    @pl.loop(0, 16)
    def _(t):
        tile = pl.ds(pl.multiple_of(t * TILE, TILE), TILE)
        xd_copy(t, 0).wait()
        xd_copy(t, 1).wait()
        xt, yt = ring.at[lax.rem(2 * t, 3)], ring.at[lax.rem(2 * t + 1, 3)]
        dwg[tile, :] = dot(xt[...], dg[...], 0, 0).astype(bf16)
        dwu[tile, :] = dot(xt[...], du[...], 0, 0).astype(bf16)

        @pl.when(t < 15)
        def _():
            xd_copy(t + 1, 1).start()

        exchanges(t, PHASE2, "a")
        dwd[:, tile] = dot(hid[...], yt[...], 0, 0).astype(bf16)

        @pl.when(t < 14)
        def _():
            xd_copy(t + 2, 0).start()

        exchanges(t, PHASE2, "b")

    for name, k in LAST:
        EVENTS[name](k)

    @pl.loop(0, CHUNKS)
    def _(k):
        for g in GROUPS:
            for kind in range(4, 10):
                if kind >= 7:
                    copy_of(kind, k, g).wait_recv()
                copy_of(kind, k, g).wait_send()

    for g in GROUPS:
        for kind in range(1, 4):
            copy_of(kind, CHUNKS - 1, g).wait_send()


def solution(mesh):
    hbm = pl.BlockSpec(memory_space=pltpu.HBM)
    vmem = pl.BlockSpec(memory_space=pltpu.VMEM)
    sem = pltpu.SemaphoreType.DMA

    def step(*args):
        return tuple(pl.pallas_call(
            kernel,
            out_shape=[pltpu.VMEM(s, bf16) for s in ((ROWS, D), (D, FF), (D, FF), (FF, D))],
            in_specs=[hbm] * 7,
            out_specs=[vmem] * 4,
            scratch_shapes=[
                pltpu.VMEM((ROWS, FF), bf16),
                pltpu.VMEM((ROWS, FF), bf16),
                pltpu.VMEM((ROWS, FF), bf16),
                pltpu.VMEM((R, D), bf16),
                pltpu.VMEM((3, ROWS, TILE), bf16),
                pltpu.VMEM((R, HALF), f32),
                pltpu.VMEM((2, 128, HALF), f32),
                pltpu.VMEM((4, 64, HALF), f32),
                pltpu.VMEM((128, HALF), bf16),
                pltpu.VMEM((64, HALF), bf16),
                pltpu.VMEM((32, HALF), bf16),
                pltpu.VMEM((CHUNKS, 128, HALF), bf16),
                sem((3,)), sem((3, 2)), sem((3,)),
                sem((10, CHUNKS, 3)), sem((10, CHUNKS, 3)), pltpu.SemaphoreType.REGULAR((CHUNKS,)),
            ],
            compiler_params=pltpu.CompilerParams(collective_id=0, has_side_effects=True, vmem_limit_bytes=VMEM_LIMIT),
        )(*args))

    tokens, columns, rows = P("dp", None), P(None, "tp"), P("tp", None)
    return jax.shard_map(
        step,
        mesh=mesh,
        in_specs=(tokens, tokens, P("dp", "tp"), P("dp", "tp"), columns, columns, rows),
        out_specs=(tokens, P("dp", "tp"), P("dp", "tp"), P(("dp", "tp"), None)),
        check_vma=False,
    )


VMEM_LIMIT = 31_391_744
```

```python
import jax
import jax.numpy as jnp
from jax import lax
from jax.experimental import pallas as pl
from jax.experimental.pallas import tpu as pltpu
from jax.sharding import PartitionSpec as P

bf16, f32 = jnp.bfloat16, jnp.float32
MESH = pl.DeviceIdType.MESH
ROWS, D, FF = 2048, 4096, 768
CHUNKS, R = 8, 256
HALF = D // 2
OFF, WIDTH = (0, 768, 1536), (768, 768, 512)
GROUPS = range(3)
TILE = 256
STRIP = 16
NB = 1024
KEPT = 4
PHASE1 = {
    (1, "o"): [("rs1", 0)],
    (2, "o"): [("rs1", 1)],
    (3, "b"): [("rs2", 0)],
    (3, "o"): [("rs1", 2)],
    (4, "b"): [("rs3", 0), ("rs2", 1)],
    (4, "o"): [("rs1", 3)],
    (5, "b"): [("rs2", 2), ("ag3", 0)],
    (5, "g"): [("rs3", 1)],
    (5, "o"): [("rs1", 4)],
    (6, "b"): [("rs2", 3), ("rs3", 2)],
    (6, "g"): [("ag2", 0)],
    (6, "o"): [("ag3", 1)],
    (7, "b"): [("rs1", 5)],
    (7, "o"): [("rs3", 3), ("rs2", 4)],
}
PHASE2 = {
    (0, "a"): [("ag3", 2), ("ag1", 0)],
    (0, "b"): [("rs1", 6), ("ag2", 1)],
    (2, "b"): [("rs2", 5)],
    (3, "a"): [("rs3", 4), ("ag3", 3)],
    (4, "a"): [("rs1", 7), ("ag2", 2)],
    (5, "b"): [("rs2", 6)],
    (6, "a"): [("rs3", 5), ("ag1", 1)],
    (6, "b"): [("ag3", 4)],
    (7, "a"): [("ag2", 3)],
    (8, "a"): [("rs2", 7)],
    (8, "b"): [("ag1", 2)],
    (9, "a"): [("rs3", 6), ("ag3", 5)],
    (10, "a"): [("ag2", 4)],
    (11, "a"): [("ag1", 3), ("rs3", 7)],
    (11, "b"): [("ag3", 6)],
    (12, "a"): [("ag2", 5)],
    (13, "b"): [("ag1", 4)],
    (14, "a"): [("ag3", 7)],
    (14, "b"): [("ag2", 6)],
    (15, "b"): [("ag1", 5)],
}
LAST = [("ag2", 7), ("ag1", 6), ("ag1", 7)]


def dot(a, b, ca, cb):
    return lax.dot_general(a, b, (((ca,), (cb,)), ((), ())), preferred_element_type=f32)


def kernel(
    x, dy, gate, up, wg, wu, wd,
    dx, dwg, dwu, dwd,
    dg, du, hid, dyb, ring, acc, kp1, kp2, s1, s2, s3, r1,
    dy_sem, wd_sem, w_sem, xd_sem, ss, rs, free,
):
    me = lax.axis_index("tp")
    core = lax.rem(me, 2)
    bits = tuple(lax.rem(me // s, 2) for s in (8, 4, 2))
    other = me + 1 - 2 * core

    def pick(r, values):
        return jnp.where(r == 0, values[0], jnp.where(r == 1, values[1], values[2]))

    peers = tuple(me + s * (1 - 2 * b) for s, b in zip((8, 4, 2), bits))

    def chunk_copies(k):
        rows = pl.ds(pl.multiple_of(k * R, R), R)
        return [
            pltpu.make_async_copy(dy.at[rows, :], dyb, dy_sem.at[0]),
            pltpu.make_async_copy(gate.at[rows, :], hid.at[rows, :], dy_sem.at[1]),
            pltpu.make_async_copy(up.at[rows, :], du.at[rows, :], dy_sem.at[2]),
        ]

    def w_copies(half, j):
        rows = pl.ds(pl.multiple_of(half * HALF + j * NB, NB), NB)
        where = half * (HALF // NB) + j
        return [pltpu.make_async_copy(a.at[rows, :], b.at[rows, :], w_sem.at[where, n]) for n, (a, b) in enumerate(((wg, dwg), (wu, dwu)))]

    def xd_copy(t, which):
        i = 2 * t + which
        cols = pl.ds(pl.multiple_of(t * TILE, TILE), TILE)
        return pltpu.make_async_copy((x, dy)[which].at[:, cols], ring.at[lax.rem(i, 3)], xd_sem.at[lax.rem(i, 3)])

    def wd_copy(n):
        rows = pl.ds(n * TILE, TILE)
        return pltpu.make_async_copy(wd.at[rows, :], dwd.at[rows, :], wd_sem.at[n])

    first = chunk_copies(0)
    first[0].start()
    for n in range(3):
        wd_copy(n).start()
    first[1].start()
    first[2].start()
    barrier = pltpu.get_barrier_semaphore()
    for p in peers + (other,):
        pl.semaphore_signal(barrier, inc=1, device_id={"tp": p}, device_id_type=MESH)
    pl.semaphore_wait(barrier, 4)

    def remote(kind, k, g, src, dst, to):
        return pltpu.make_async_remote_copy(
            src_ref=src, dst_ref=dst, send_sem=ss.at[kind, k, g], recv_sem=rs.at[kind, k, g],
            device_id={"tp": to}, device_id_type=MESH,
        )

    def place(k, g):
        o = [lax.rem(g + k + i, 3) for i in range(3)]
        b = [pick(r, bits) for r in o]
        p = [pick(r, peers) for r in o]
        keep1 = k * R + b[0] * 128
        send1 = k * R + (1 - b[0]) * 128
        keep2, send2 = keep1 + b[1] * 64, keep1 + (1 - b[1]) * 64
        keep3, send3 = keep2 + b[2] * 32, keep2 + (1 - b[2]) * 32
        return b, p, (keep1, keep2, keep3), (send1, send2, send3)

    def mine(start, n, g):
        return dx.at[pl.ds(pl.multiple_of(start, STRIP), n), pl.ds(pl.multiple_of(core * HALF + OFF[g], 256), WIDTH[g])]

    def theirs(k, g):
        return dx.at[pl.ds(pl.multiple_of(k * R, R), R), pl.ds(pl.multiple_of((1 - core) * HALF + OFF[g], 256), WIDTH[g])]

    def copy_of(kind, k, g):
        b, p, keep, send = place(k, g)
        cols = pl.ds(OFF[g], WIDTH[g])
        if kind == 0:
            return remote(0, k, g, theirs(k, g), theirs(k, g), other)
        if kind == 1:
            return remote(1, k, g, s1.at[:, cols], r1.at[k, :, cols], p[0])
        if kind == 2:
            there = keep[0] + (1 - b[1]) * 64
            return remote(2, k, g, s2.at[:, cols], mine(there, 64, g), p[1])
        if kind == 3:
            return remote(3, k, g, s3.at[:, cols], r1.at[k, pl.ds(0, 32), cols], p[2])
        if kind == 4:
            return remote(4, k, g, mine(keep[2], 32, g), mine(keep[2], 32, g), p[2])
        if kind == 5:
            return remote(5, k, g, mine(keep[1], 64, g), mine(keep[1], 64, g), p[1])
        if kind == 6:
            return remote(6, k, g, mine(keep[0], 128, g), mine(keep[0], 128, g), p[0])
        if kind == 7:
            return remote(7, k, g, mine(keep[1], 64, g), mine(keep[1], 64, g), other)
        if kind == 8:
            return remote(8, k, g, mine(send[1], 64, g), mine(send[1], 64, g), other)
        return remote(9, k, g, mine(send[0], 128, g), mine(send[0], 128, g), other)

    def part(start, i):
        return pl.ds(pl.multiple_of(start + i, STRIP), STRIP)

    def event(kind, k, work=None, after=()):
        for g in GROUPS:
            copy_of(kind, k, g).wait_recv()
        if kind < 3 and k > 0:
            for g in GROUPS:
                copy_of(kind + 1, k - 1, g).wait_send()
        if work is not None:
            for g in GROUPS:
                work(k, g, pl.ds(OFF[g], WIDTH[g]), *place(k, g))
        for g in GROUPS:
            for n in after:
                copy_of(n, k, g).start()

    def own(k):
        for g in GROUPS:
            copy_of(0, k, g).wait_recv()

        @pl.when(k >= 1)
        def _():
            for g in GROUPS:
                copy_of(1, k - 1, g).wait_send()

        for g in GROUPS:
            b, p, keep, send = place(k, g)
            cols = pl.ds(OFF[g], WIDTH[g])
            for i in range(0, 128, STRIP):
                v = acc[part((1 - b[0]) * 128, i), cols] + mine(send[0] + i, STRIP, g)[...].astype(f32)
                s1[pl.ds(i, STRIP), cols] = v.astype(bf16)
                v = acc[part(b[0] * 128, i), cols] + mine(keep[0] + i, STRIP, g)[...].astype(f32)
                kp1[lax.rem(k, 2), pl.ds(i, STRIP), cols] = v
        for g in GROUPS:
            copy_of(1, k, g).start()

    def halve1(k, g, cols, b, p, keep, send):
        for i in range(0, 64, STRIP):
            rows = part((1 - b[1]) * 64, i)
            s2[pl.ds(i, STRIP), cols] = (kp1[k % 2, rows, cols] + r1[k, rows, cols].astype(f32)).astype(bf16)
            rows = part(b[1] * 64, i)
            kp2[k % KEPT, pl.ds(i, STRIP), cols] = kp1[k % 2, rows, cols] + r1[k, rows, cols].astype(f32)

    def halve2(k, g, cols, b, p, keep, send):
        for i in range(0, 32, STRIP):
            v = kp2[k % KEPT, part((1 - b[2]) * 32, i), cols] + mine(send[2] + i, STRIP, g)[...].astype(f32)
            s3[pl.ds(i, STRIP), cols] = v.astype(bf16)
            rows = part(b[2] * 32, i)
            kp2[k % KEPT, rows, cols] = kp2[k % KEPT, rows, cols] + mine(keep[2] + i, STRIP, g)[...].astype(f32)

    def halve3(k, g, cols, b, p, keep, send):
        for i in range(0, 32, STRIP):
            v = kp2[k % KEPT, part(b[2] * 32, i), cols] + r1[k, pl.ds(i, STRIP), cols].astype(f32)
            mine(keep[2] + i, STRIP, g)[...] = v.astype(bf16)

    def gather3(k):
        pl.semaphore_wait(free.at[k], 1)
        event(4, k, after=(5, 7))

    EVENTS = {
        "rs1": lambda k: event(1, k, halve1, (2,)),
        "rs2": lambda k: event(2, k, halve2, (3,)),
        "rs3": lambda k: event(3, k, halve3, (4,)),
        "ag3": gather3,
        "ag2": lambda k: event(5, k, after=(6, 8)),
        "ag1": lambda k: event(6, k, after=(9,)),
    }

    def exchanges(step, table, point):
        for (n, at), events in table.items():
            if at == point:
                @pl.when(step == n)
                def _():
                    for name, k in events:
                        EVENTS[name](k)

    def gradients(k):
        copies = chunk_copies(k)
        copies[0].wait()
        if isinstance(k, int) and k == 0:
            for n in range(3):
                wd_copy(n).wait()
                cols = pl.ds(n * TILE, TILE)
                acc[:, cols] = dot(dyb[...], dwd[cols, :], 1, 1)
        else:
            acc[:, pl.ds(0, FF)] = dot(dyb[...], dwd[...], 1, 1)
        copies[1].wait()
        copies[2].wait()

        @pl.loop(0, R // 16, unroll=2)
        def _(n):
            i = pl.multiple_of(n * 16, 16)
            here = pl.ds(pl.multiple_of(k * R + i, 16), 16)
            a, b, d = hid[here, :].astype(f32), du[here, :].astype(f32), acc[pl.ds(i, 16), pl.ds(0, FF)]
            sig = jax.nn.sigmoid(a)
            silu = a * sig
            hid[here, :] = (silu * b).astype(bf16)
            du[here, :] = (d * silu).astype(bf16)
            dg[here, :] = (d * b * (sig + silu * (1.0 - sig))).astype(bf16)

    def term(k, half):
        rows = pl.ds(pl.multiple_of(k * R, R), R)
        @pl.loop(0, HALF // NB)
        def _(j):
            @pl.when(k == 0)
            def _():
                for c in w_copies(half, j):
                    c.wait()

            n = pl.multiple_of(j * NB, NB)
            w = pl.ds(pl.multiple_of(half * HALF + n, 256), NB)
            t = dot(dg[rows, :], dwg[w, :], 1, 1) + dot(du[rows, :], dwu[w, :], 1, 1)
            if half is core:
                acc[:, pl.ds(n, NB)] = t
            else:
                dx[rows, w] = t.astype(bf16)

    for half in (1 - core, core):
        for j in range(HALF // NB):
            for c in w_copies(half, j):
                c.start()
    gradients(0)
    for c in chunk_copies(1):
        c.start()

    @pl.loop(0, CHUNKS)
    def _(k):
        term(k, 1 - core)
        for g in GROUPS:
            copy_of(0, k, g).start()
        exchanges(k, PHASE1, "b")

        @pl.when(k < CHUNKS - 1)
        def _():
            gradients(k + 1)

        @pl.when(k < CHUNKS - 2)
        def _():
            for c in chunk_copies(k + 2):
                c.start()

        @pl.when(k == CHUNKS - 2)
        def _():
            for i in range(3):
                xd_copy(i // 2, i % 2).start()

        exchanges(k, PHASE1, "g")

        term(k, core)
        own(k)
        for g in GROUPS:
            copy_of(0, k, g).wait_send()
        pl.semaphore_signal(free.at[k], inc=1, device_id={"tp": other}, device_id_type=MESH)
        exchanges(k, PHASE1, "o")

    @pl.loop(0, 16)
    def _(t):
        tile = pl.ds(pl.multiple_of(t * TILE, TILE), TILE)
        xd_copy(t, 0).wait()
        xd_copy(t, 1).wait()
        xt, yt = ring.at[lax.rem(2 * t, 3)], ring.at[lax.rem(2 * t + 1, 3)]
        dwg[tile, :] = dot(xt[...], dg[...], 0, 0).astype(bf16)
        dwu[tile, :] = dot(xt[...], du[...], 0, 0).astype(bf16)

        @pl.when(t < 15)
        def _():
            xd_copy(t + 1, 1).start()

        exchanges(t, PHASE2, "a")
        dwd[:, tile] = dot(hid[...], yt[...], 0, 0).astype(bf16)

        @pl.when(t < 14)
        def _():
            xd_copy(t + 2, 0).start()

        exchanges(t, PHASE2, "b")

    for name, k in LAST:
        EVENTS[name](k)

    @pl.loop(0, CHUNKS)
    def _(k):
        for g in GROUPS:
            for kind in range(4, 10):
                if kind >= 7:
                    copy_of(kind, k, g).wait_recv()
                copy_of(kind, k, g).wait_send()

    for g in GROUPS:
        for kind in range(1, 4):
            copy_of(kind, CHUNKS - 1, g).wait_send()


def write_out(*arrays):
    n = len(arrays)

    def copies(*refs):
        out = [
            pltpu.make_async_copy(a.at[rows], b.at[rows], refs[-1].at[4 * i + q])
            for i, (a, b) in enumerate(zip(refs[:n], refs[n : 2 * n]))
            for q in range(4)
            for rows in [pl.ds(q * (a.shape[0] // 4), a.shape[0] // 4)]
        ]
        for c in out:
            c.start()
        for c in out:
            c.wait()

    return pl.pallas_call(
        copies,
        out_shape=[jax.ShapeDtypeStruct(a.shape, a.dtype) for a in arrays],
        in_specs=[pl.BlockSpec(memory_space=pltpu.VMEM)] * n,
        out_specs=[pl.BlockSpec(memory_space=pl.ANY)] * n,
        scratch_shapes=[pltpu.SemaphoreType.DMA((4 * n,))],
        compiler_params=pltpu.CompilerParams(vmem_limit_bytes=1024),
    )(*arrays)


def solution(mesh):
    hbm = pl.BlockSpec(memory_space=pltpu.HBM)
    vmem = pl.BlockSpec(memory_space=pltpu.VMEM)
    sem = pltpu.SemaphoreType.DMA

    def step(*args):
        dx, *dw = pl.pallas_call(
            kernel,
            out_shape=[pltpu.VMEM(s, bf16) for s in ((ROWS, D), (D, FF), (D, FF), (FF, D))],
            in_specs=[hbm] * 7,
            out_specs=[vmem] * 4,
            scratch_shapes=[
                pltpu.VMEM((ROWS, FF), bf16),
                pltpu.VMEM((ROWS, FF), bf16),
                pltpu.VMEM((ROWS, FF), bf16),
                pltpu.VMEM((R, D), bf16),
                pltpu.VMEM((3, ROWS, TILE), bf16),
                pltpu.VMEM((R, HALF), f32),
                pltpu.VMEM((2, 128, HALF), f32),
                pltpu.VMEM((4, 64, HALF), f32),
                pltpu.VMEM((128, HALF), bf16),
                pltpu.VMEM((64, HALF), bf16),
                pltpu.VMEM((32, HALF), bf16),
                pltpu.VMEM((CHUNKS, 128, HALF), bf16),
                sem((3,)), sem((3,)), sem((D // NB, 2)), sem((3,)),
                sem((10, CHUNKS, 3)), sem((10, CHUNKS, 3)), pltpu.SemaphoreType.REGULAR((CHUNKS,)),
            ],
            compiler_params=pltpu.CompilerParams(collective_id=0, has_side_effects=True, vmem_limit_bytes=VMEM_LIMIT),
        )(*args)
        return (*write_out(dx), *write_out(*dw))

    tokens, columns, rows = P("dp", None), P(None, "tp"), P("tp", None)
    return jax.shard_map(
        step,
        mesh=mesh,
        in_specs=(tokens, tokens, P("dp", "tp"), P("dp", "tp"), columns, columns, rows),
        out_specs=(tokens, P("dp", "tp"), P("dp", "tp"), P(("dp", "tp"), None)),
        check_vma=False,
    )


VMEM_LIMIT = 31_391_744
```

```python
import jax
import jax.numpy as jnp
from jax import lax
from jax.experimental import pallas as pl
from jax.experimental.pallas import tpu as pltpu
from jax.sharding import PartitionSpec as P

bf16, f32 = jnp.bfloat16, jnp.float32
MESH = pl.DeviceIdType.MESH
ROWS, D, FF = 2048, 4096, 768
CHUNKS, R = 8, 256
HALF = D // 2
OFF, WIDTH = (0, 768, 1536), (768, 768, 512)
GROUPS = range(3)
TILE = 256
STRIP = 16
NB = 1024
KEPT = 4
PHASE1 = {
    (1, "o"): [("rs1", 0)],
    (2, "o"): [("rs1", 1)],
    (3, "b"): [("rs2", 0)],
    (3, "o"): [("rs1", 2)],
    (4, "b"): [("rs3", 0), ("rs2", 1)],
    (4, "o"): [("rs1", 3)],
    (5, "b"): [("rs2", 2), ("ag3", 0)],
    (5, "g"): [("rs3", 1)],
    (5, "o"): [("rs1", 4)],
    (6, "b"): [("rs2", 3), ("rs3", 2)],
    (6, "g"): [("ag2", 0)],
    (6, "o"): [("ag3", 1)],
    (7, "b"): [("rs1", 5)],
    (7, "o"): [("rs3", 3), ("rs2", 4)],
}
PHASE2 = {
    (0, "a"): [("ag3", 2), ("ag1", 0)],
    (0, "b"): [("rs1", 6), ("ag2", 1)],
    (2, "b"): [("rs2", 5)],
    (3, "a"): [("rs3", 4), ("ag3", 3)],
    (4, "a"): [("rs1", 7), ("ag2", 2)],
    (5, "b"): [("rs2", 6)],
    (6, "a"): [("rs3", 5), ("ag1", 1)],
    (6, "b"): [("ag3", 4)],
    (7, "a"): [("ag2", 3)],
    (8, "a"): [("rs2", 7)],
    (8, "b"): [("ag1", 2)],
    (9, "a"): [("rs3", 6), ("ag3", 5)],
    (10, "a"): [("ag2", 4)],
    (11, "a"): [("ag1", 3), ("rs3", 7)],
    (11, "b"): [("ag3", 6)],
    (12, "a"): [("ag2", 5)],
    (13, "b"): [("ag1", 4)],
    (14, "a"): [("ag3", 7)],
    (14, "b"): [("ag2", 6)],
    (15, "b"): [("ag1", 5)],
}
LAST = [("ag2", 7), ("ag1", 6), ("ag1", 7)]


def dot(a, b, ca, cb):
    return lax.dot_general(a, b, (((ca,), (cb,)), ((), ())), preferred_element_type=f32)


def kernel(
    x, dy, gate, up, wg, wu, wd,
    dx, dwg, dwu, dwd,
    dg, du, hid, dyb, ring, acc, kp1, kp2, s1, s2, s3, r1,
    dy_sem, wd_sem, w_sem, xd_sem, ss, rs, free,
):
    me = lax.axis_index("tp")
    core = lax.rem(me, 2)
    bits = tuple(lax.rem(me // s, 2) for s in (8, 4, 2))
    other = me + 1 - 2 * core

    def pick(r, values):
        return jnp.where(r == 0, values[0], jnp.where(r == 1, values[1], values[2]))

    peers = tuple(me + s * (1 - 2 * b) for s, b in zip((8, 4, 2), bits))

    def chunk_copies(k):
        rows = pl.ds(pl.multiple_of(k * R, R), R)
        return [
            pltpu.make_async_copy(dy.at[rows, :], dyb, dy_sem.at[0]),
            pltpu.make_async_copy(gate.at[rows, :], hid.at[rows, :], dy_sem.at[1]),
            pltpu.make_async_copy(up.at[rows, :], du.at[rows, :], dy_sem.at[2]),
        ]

    def w_copies(half, j):
        rows = pl.ds(pl.multiple_of(half * HALF + j * NB, NB), NB)
        where = half * (HALF // NB) + j
        return [pltpu.make_async_copy(a.at[rows, :], b.at[rows, :], w_sem.at[where, n]) for n, (a, b) in enumerate(((wg, dwg), (wu, dwu)))]

    def xd_copy(t, which):
        i = 2 * t + which
        cols = pl.ds(pl.multiple_of(t * TILE, TILE), TILE)
        return pltpu.make_async_copy((x, dy)[which].at[:, cols], ring.at[lax.rem(i, 3)], xd_sem.at[lax.rem(i, 3)])

    def wd_copy(n):
        rows = pl.ds(n * TILE, TILE)
        return pltpu.make_async_copy(wd.at[rows, :], dwd.at[rows, :], wd_sem.at[n])

    first = chunk_copies(0)
    first[0].start()
    for n in range(3):
        wd_copy(n).start()
    first[1].start()
    first[2].start()
    barrier = pltpu.get_barrier_semaphore()
    for p in peers + (other,):
        pl.semaphore_signal(barrier, inc=1, device_id={"tp": p}, device_id_type=MESH)
    pl.semaphore_wait(barrier, 4)

    def remote(kind, k, g, src, dst, to):
        return pltpu.make_async_remote_copy(
            src_ref=src, dst_ref=dst, send_sem=ss.at[kind, k, g], recv_sem=rs.at[kind, k, g],
            device_id={"tp": to}, device_id_type=MESH,
        )

    def place(k, g):
        o = [lax.rem(g + k + i, 3) for i in range(3)]
        b = [pick(r, bits) for r in o]
        p = [pick(r, peers) for r in o]
        keep1 = k * R + b[0] * 128
        send1 = k * R + (1 - b[0]) * 128
        keep2, send2 = keep1 + b[1] * 64, keep1 + (1 - b[1]) * 64
        keep3, send3 = keep2 + b[2] * 32, keep2 + (1 - b[2]) * 32
        return b, p, (keep1, keep2, keep3), (send1, send2, send3)

    def mine(start, n, g):
        return dx.at[pl.ds(pl.multiple_of(start, STRIP), n), pl.ds(pl.multiple_of(core * HALF + OFF[g], 256), WIDTH[g])]

    def theirs(k, g):
        return dx.at[pl.ds(pl.multiple_of(k * R, R), R), pl.ds(pl.multiple_of((1 - core) * HALF + OFF[g], 256), WIDTH[g])]

    def copy_of(kind, k, g):
        b, p, keep, send = place(k, g)
        cols = pl.ds(OFF[g], WIDTH[g])
        if kind == 0:
            return remote(0, k, g, theirs(k, g), theirs(k, g), other)
        if kind == 1:
            return remote(1, k, g, s1.at[:, cols], r1.at[k, :, cols], p[0])
        if kind == 2:
            there = keep[0] + (1 - b[1]) * 64
            return remote(2, k, g, s2.at[:, cols], mine(there, 64, g), p[1])
        if kind == 3:
            return remote(3, k, g, s3.at[:, cols], r1.at[k, pl.ds(0, 32), cols], p[2])
        if kind == 4:
            return remote(4, k, g, mine(keep[2], 32, g), mine(keep[2], 32, g), p[2])
        if kind == 5:
            return remote(5, k, g, mine(keep[1], 64, g), mine(keep[1], 64, g), p[1])
        if kind == 6:
            return remote(6, k, g, mine(keep[0], 128, g), mine(keep[0], 128, g), p[0])
        if kind == 7:
            return remote(7, k, g, mine(keep[1], 64, g), mine(keep[1], 64, g), other)
        if kind == 8:
            return remote(8, k, g, mine(send[1], 64, g), mine(send[1], 64, g), other)
        return remote(9, k, g, mine(send[0], 128, g), mine(send[0], 128, g), other)

    def part(start, i):
        return pl.ds(pl.multiple_of(start + i, STRIP), STRIP)

    def event(kind, k, work=None, after=()):
        for g in GROUPS:
            copy_of(kind, k, g).wait_recv()
        if kind < 3 and k > 0:
            for g in GROUPS:
                copy_of(kind + 1, k - 1, g).wait_send()
        if work is not None:
            for g in GROUPS:
                work(k, g, pl.ds(OFF[g], WIDTH[g]), *place(k, g))
        for g in GROUPS:
            for n in after:
                copy_of(n, k, g).start()

    def own(k):
        for g in GROUPS:
            copy_of(0, k, g).wait_recv()

        @pl.when(k >= 1)
        def _():
            for g in GROUPS:
                copy_of(1, k - 1, g).wait_send()

        for g in GROUPS:
            b, p, keep, send = place(k, g)
            cols = pl.ds(OFF[g], WIDTH[g])
            for i in range(0, 128, STRIP):
                v = acc[part((1 - b[0]) * 128, i), cols] + mine(send[0] + i, STRIP, g)[...].astype(f32)
                s1[pl.ds(i, STRIP), cols] = v.astype(bf16)
                v = acc[part(b[0] * 128, i), cols] + mine(keep[0] + i, STRIP, g)[...].astype(f32)
                kp1[lax.rem(k, 2), pl.ds(i, STRIP), cols] = v
        for g in GROUPS:
            copy_of(1, k, g).start()

    def halve1(k, g, cols, b, p, keep, send):
        for i in range(0, 64, STRIP):
            rows = part((1 - b[1]) * 64, i)
            s2[pl.ds(i, STRIP), cols] = (kp1[k % 2, rows, cols] + r1[k, rows, cols].astype(f32)).astype(bf16)
            rows = part(b[1] * 64, i)
            kp2[k % KEPT, pl.ds(i, STRIP), cols] = kp1[k % 2, rows, cols] + r1[k, rows, cols].astype(f32)

    def halve2(k, g, cols, b, p, keep, send):
        for i in range(0, 32, STRIP):
            v = kp2[k % KEPT, part((1 - b[2]) * 32, i), cols] + mine(send[2] + i, STRIP, g)[...].astype(f32)
            s3[pl.ds(i, STRIP), cols] = v.astype(bf16)
            rows = part(b[2] * 32, i)
            kp2[k % KEPT, rows, cols] = kp2[k % KEPT, rows, cols] + mine(keep[2] + i, STRIP, g)[...].astype(f32)

    def halve3(k, g, cols, b, p, keep, send):
        for i in range(0, 32, STRIP):
            v = kp2[k % KEPT, part(b[2] * 32, i), cols] + r1[k, pl.ds(i, STRIP), cols].astype(f32)
            mine(keep[2] + i, STRIP, g)[...] = v.astype(bf16)

    def gather3(k):
        pl.semaphore_wait(free.at[k], 1)
        event(4, k, after=(5, 7))

    EVENTS = {
        "rs1": lambda k: event(1, k, halve1, (2,)),
        "rs2": lambda k: event(2, k, halve2, (3,)),
        "rs3": lambda k: event(3, k, halve3, (4,)),
        "ag3": gather3,
        "ag2": lambda k: event(5, k, after=(6, 8)),
        "ag1": lambda k: event(6, k, after=(9,)),
    }

    def exchanges(step, table, point):
        for (n, at), events in table.items():
            if at == point:
                @pl.when(step == n)
                def _():
                    for name, k in events:
                        EVENTS[name](k)

    def gradients(k):
        copies = chunk_copies(k)
        copies[0].wait()
        if isinstance(k, int) and k == 0:
            for n in range(3):
                wd_copy(n).wait()
                cols = pl.ds(n * TILE, TILE)
                acc[:, cols] = dot(dyb[...], dwd[cols, :], 1, 1)
        else:
            acc[:, pl.ds(0, FF)] = dot(dyb[...], dwd[...], 1, 1)
        copies[1].wait()
        copies[2].wait()

        @pl.loop(0, R // 16, unroll=2)
        def _(n):
            i = pl.multiple_of(n * 16, 16)
            here = pl.ds(pl.multiple_of(k * R + i, 16), 16)
            a, b, d = hid[here, :].astype(f32), du[here, :].astype(f32), acc[pl.ds(i, 16), pl.ds(0, FF)]
            sig = jax.nn.sigmoid(a)
            silu = a * sig
            hid[here, :] = (silu * b).astype(bf16)
            du[here, :] = (d * silu).astype(bf16)
            dg[here, :] = (d * b * (sig + silu * (1.0 - sig))).astype(bf16)

    def term(k, half):
        rows = pl.ds(pl.multiple_of(k * R, R), R)
        @pl.loop(0, HALF // NB)
        def _(j):
            @pl.when(k == 0)
            def _():
                for c in w_copies(half, j):
                    c.wait()

            n = pl.multiple_of(j * NB, NB)
            w = pl.ds(pl.multiple_of(half * HALF + n, 256), NB)
            t = dot(dg[rows, :], dwg[w, :], 1, 1) + dot(du[rows, :], dwu[w, :], 1, 1)
            if half is core:
                acc[:, pl.ds(n, NB)] = t
            else:
                dx[rows, w] = t.astype(bf16)

    for half in (1 - core, core):
        for j in range(HALF // NB):
            for c in w_copies(half, j):
                c.start()
    gradients(0)
    for c in chunk_copies(1):
        c.start()

    @pl.loop(0, CHUNKS)
    def _(k):
        term(k, 1 - core)
        for g in GROUPS:
            copy_of(0, k, g).start()
        exchanges(k, PHASE1, "b")

        @pl.when(k < CHUNKS - 1)
        def _():
            gradients(k + 1)

        @pl.when(k < CHUNKS - 2)
        def _():
            for c in chunk_copies(k + 2):
                c.start()

        @pl.when(k == CHUNKS - 2)
        def _():
            for i in range(3):
                xd_copy(i // 2, i % 2).start()

        exchanges(k, PHASE1, "g")

        term(k, core)
        own(k)
        for g in GROUPS:
            copy_of(0, k, g).wait_send()
        pl.semaphore_signal(free.at[k], inc=1, device_id={"tp": other}, device_id_type=MESH)
        exchanges(k, PHASE1, "o")

    @pl.loop(0, 16)
    def _(t):
        tile = pl.ds(pl.multiple_of(t * TILE, TILE), TILE)
        xd_copy(t, 0).wait()
        xd_copy(t, 1).wait()
        xt, yt = ring.at[lax.rem(2 * t, 3)], ring.at[lax.rem(2 * t + 1, 3)]
        dwg[tile, :] = dot(xt[...], dg[...], 0, 0).astype(bf16)
        dwu[tile, :] = dot(xt[...], du[...], 0, 0).astype(bf16)

        @pl.when(t < 15)
        def _():
            xd_copy(t + 1, 1).start()

        exchanges(t, PHASE2, "a")
        dwd[:, tile] = dot(hid[...], yt[...], 0, 0).astype(bf16)

        @pl.when(t < 14)
        def _():
            xd_copy(t + 2, 0).start()

        exchanges(t, PHASE2, "b")

    def finish(k):
        for g in GROUPS:
            for kind in range(4, 10):
                if kind >= 7:
                    copy_of(kind, k, g).wait_recv()
                copy_of(kind, k, g).wait_send()

    first = 1 + max(i for i, (name, _) in enumerate(LAST) if name != "ag1")
    for name, k in LAST[:first]:
        EVENTS[name](k)
    for g in GROUPS:
        for kind in range(1, 4):
            copy_of(kind, CHUNKS - 1, g).wait_send()

    @pl.loop(0, min(k for name, k in LAST if name == "ag1"))
    def _(k):
        finish(k)

    for name, k in LAST[first:]:
        EVENTS[name](k)
    for name, k in LAST:
        if name == "ag1":
            finish(k)


def write_out(*arrays):
    n = len(arrays)

    def copies(*refs):
        out = [
            pltpu.make_async_copy(a.at[rows], b.at[rows], refs[-1].at[8 * i + q])
            for i, (a, b) in enumerate(zip(refs[:n], refs[n : 2 * n]))
            for q in range(8)
            for rows in [pl.ds(q * (a.shape[0] // 8), a.shape[0] // 8)]
        ]
        for c in out:
            c.start()
        for c in out:
            c.wait()

    return pl.pallas_call(
        copies,
        out_shape=[jax.ShapeDtypeStruct(a.shape, a.dtype) for a in arrays],
        in_specs=[pl.BlockSpec(memory_space=pltpu.VMEM)] * n,
        out_specs=[pl.BlockSpec(memory_space=pl.ANY)] * n,
        scratch_shapes=[pltpu.SemaphoreType.DMA((8 * n,))],
        compiler_params=pltpu.CompilerParams(vmem_limit_bytes=1024),
    )(*arrays)


def solution(mesh):
    hbm = pl.BlockSpec(memory_space=pltpu.HBM)
    vmem = pl.BlockSpec(memory_space=pltpu.VMEM)
    sem = pltpu.SemaphoreType.DMA

    def step(*args):
        dx, *dw = pl.pallas_call(
            kernel,
            out_shape=[pltpu.VMEM(s, bf16) for s in ((ROWS, D), (D, FF), (D, FF), (FF, D))],
            in_specs=[hbm] * 7,
            out_specs=[vmem] * 4,
            scratch_shapes=[
                pltpu.VMEM((ROWS, FF), bf16),
                pltpu.VMEM((ROWS, FF), bf16),
                pltpu.VMEM((ROWS, FF), bf16),
                pltpu.VMEM((R, D), bf16),
                pltpu.VMEM((3, ROWS, TILE), bf16),
                pltpu.VMEM((R, HALF), f32),
                pltpu.VMEM((2, 128, HALF), f32),
                pltpu.VMEM((4, 64, HALF), f32),
                pltpu.VMEM((128, HALF), bf16),
                pltpu.VMEM((64, HALF), bf16),
                pltpu.VMEM((32, HALF), bf16),
                pltpu.VMEM((CHUNKS, 128, HALF), bf16),
                sem((3,)), sem((3,)), sem((D // NB, 2)), sem((3,)),
                sem((10, CHUNKS, 3)), sem((10, CHUNKS, 3)), pltpu.SemaphoreType.REGULAR((CHUNKS,)),
            ],
            compiler_params=pltpu.CompilerParams(collective_id=0, has_side_effects=True, vmem_limit_bytes=VMEM_LIMIT),
        )(*args)
        return (*write_out(dx), *write_out(*dw))

    tokens, columns, rows = P("dp", None), P(None, "tp"), P("tp", None)
    return jax.shard_map(
        step,
        mesh=mesh,
        in_specs=(tokens, tokens, P("dp", "tp"), P("dp", "tp"), columns, columns, rows),
        out_specs=(tokens, P("dp", "tp"), P("dp", "tp"), P(("dp", "tp"), None)),
        check_vma=False,
    )


VMEM_LIMIT = 31_391_744
```
